128 devices in a mesh: layer: 8 (over y_hi, x), width: 16 (over y_lo, z, core).
Axes of the slice: x: 4, y: 4 (y_hi: 2, y_lo: 2; y = y_hi * 2 + y_lo), z: 4, core: 2. Of those that a mesh axis runs over, the one named last changes fastest.
Arguments:
- source: bfloat16 [8, 4096, 4096], P('layer', 'width'), may hold values from -6 to 6
- expand_out: bfloat16 [2560, 4096], P(None, 'width'), may hold values from -0.125 to 0.125
- expand_in: bfloat16 [2560, 4096], P(('layer', 'width')), may hold values from -0.09375 to 0.09375
- depth: float32 [16, 8], P('layer'), may hold values from -1.4 to 1.4
Outputs:
- grown: float32 [16, 2560, 2560], P('layer', 'width')
The draws below stay inside these ranges and needn't reach their ends.
All inputs are finite; a program needn't handle non-finite values.
Results may differ from the reference program's by a relative error of at most 0.018.
Values may be sent and summed in bfloat16 or wider, within the bound.
A program may use at most 128 MiB of HBM per device.

```python
import jax
import jax.numpy as jnp
from jax import lax

D1 = 4096
R = 2560
C = 2560
SRC = 8
TGT = 16
N_WIDTH = 16


def spiked(values, own_key, source, target, blocks, factor):
    def block_of(axis_at):
        return (jnp.arange(values.shape[axis_at]) // (values.shape[axis_at] // blocks)).reshape((-1,) + (1,) * (values.ndim - 1 - axis_at))

    one_side = jax.random.permutation(own_key, blocks)[block_of(target)]
    other_side = (block_of(target) + blocks // 2) % blocks
    return jnp.where((block_of(source) == one_side) | (block_of(source) == other_side), factor * values, values)


def shard_levels(stream_key, extent, split, smallest, largest):
    def one(axis_at, parts):
        heights = jax.random.uniform(jax.random.fold_in(jax.random.fold_in(stream_key, 6), axis_at), (parts,), jnp.float32, smallest / len(split), largest / len(split))
        return jnp.repeat(jnp.exp(heights), extent[axis_at] // parts).reshape((-1,) + (1,) * (len(extent) - axis_at - 1))

    gain = one(*split[0])
    for cut in split[1:]:
        gain = gain * one(*cut)
    return gain


def centred(rng, shape, spread, reach, pieces=(), dtype=jnp.bfloat16):
    loudness = shard_levels(rng, shape, pieces, -0.22, 0.18) if pieces else 1.0
    values = jax.random.normal(rng, shape, jnp.float32) * spread * loudness
    return jnp.minimum(jnp.maximum(values, -reach), reach).astype(dtype)


def bell_draw_with(own_key, shape, deviation, most, cuts, heavy, held_as=jnp.bfloat16):
    values = deviation * jax.random.normal(own_key, shape, jnp.float32)
    if cuts:
        values = values * shard_levels(own_key, shape, cuts, -0.22, 0.18)
    return jnp.clip(spiked(values, jax.random.fold_in(own_key, 3), *heavy), -most, most).astype(held_as)


def setup_inputs(seed: int = 0) -> dict:
    streams_of = jax.random.split(jax.random.key(seed), 5)
    return {
        "source": centred(streams_of[0], (SRC, D1, D1), 1.0, 6.0, ((0, 8), (1, 16))),
        "expand_out": bell_draw_with(streams_of[1], (R, D1), D1 ** -0.5, 0.125, ((1, 16),), (1, 0, 16, 2.0)),
        "expand_in": centred(streams_of[2], (C, D1), D1 ** -0.5, 0.09375, ((0, 128),)),
        "depth": centred(streams_of[3], (TGT, SRC), 0.35, 1.4, ((0, 8),), jnp.float32),
    }


def reference(source, expand_out, expand_in, depth):
    block_count = N_WIDTH
    block_width = D1 // block_count

    def expand(weight):
        projected = jnp.dot(weight, expand_in.T, preferred_element_type=jnp.float32).astype(jnp.bfloat16)

        def add_block(block_index, running):
            first_row = (block_index * block_width).astype(jnp.int32)
            inner_rows = lax.dynamic_slice_in_dim(projected, first_row, block_width, 0)
            outer_cols = lax.dynamic_slice_in_dim(expand_out, first_row, block_width, 1)
            partial_value = jnp.dot(outer_cols, inner_rows, preferred_element_type=jnp.float32).astype(jnp.bfloat16)
            partial_value = lax.optimization_barrier(partial_value)
            return running + partial_value.astype(jnp.float32)

        running = lax.fori_loop(0, block_count, add_block, jnp.zeros((R, C), jnp.float32))
        return running.astype(jnp.bfloat16)

    expanded = lax.map(expand, source)
    stacked = expanded.astype(jnp.float32).reshape(SRC, R * C)
    grown = jnp.dot(depth, stacked, precision=lax.Precision.HIGHEST, preferred_element_type=jnp.float32)
    return grown.reshape(TGT, R, C)
```

```python
import jax
import jax.numpy as jnp
from jax import lax
from jax.experimental import pallas as pl
from jax.experimental.pallas import tpu as pltpu
from jax.sharding import Mesh
from jax.sharding import PartitionSpec as P

AXES = ("hi", "x", "lo", "z", "c")
NS = 5
NT = (((1,), (1,)), ((), ()))
F32 = jnp.float32
BF16 = jnp.bfloat16


def mod(value, n):
    return lax.rem(value, n)


def kernel(
    src, eo_in, e_in, depth, out,
    zbuf, eb, sb, eo, pt, pbuf, lbuf, rbuf, rel, zf, ra, bs, xq, xg, tb, fin, d_oth, cf,
    send, recv, loc,
):
    hi, x, lo, z, c = (lax.axis_index(a) for a in AXES)
    y = hi * 2 + lo

    def dev(dx=0, dy=0, dz=0, core=None):
        ny = mod(y + dy + 4, 4)
        return (
            lax.div(ny, 2), mod(x + dx + 4, 4), mod(ny, 2), mod(z + dz + 4, 4),
            c if core is None else core,
        )

    a_side = (hi, x, 1 - lo, z)
    b_side = (1 - hi, x, 1 - lo, z)
    partner = dev(core=1 - c)

    count = [0]
    started = []

    def remote(src_ref, dst_ref, device, slot=None):
        i = count[0]
        count[0] += 1
        return pltpu.make_async_remote_copy(
            src_ref=src_ref, dst_ref=dst_ref, send_sem=send.at[i],
            recv_sem=recv.at[i] if slot is None else recv.at[slot],
            device_id=device, device_id_type=pl.DeviceIdType.MESH,
        )

    def go(copy):
        copy.start()
        started.append(copy)
        return copy

    barrier = pltpu.get_barrier_semaphore()
    peers = [dev(dx=d) for d in (1, -1, 2)] + [dev(dy=2)] + [dev(dz=d) for d in (1, -1, 2)] + [partner]
    peers += [a_side + (k,) for k in (0, 1)] + [b_side + (k,) for k in (0, 1)]
    for peer in peers:
        pl.semaphore_signal(barrier, inc=1, device_id=peer, device_id_type=pl.DeviceIdType.MESH)
    pl.semaphore_wait(barrier, len(peers))

    zloc = pltpu.make_async_copy(e_in, zbuf.at[z], loc.at[0])
    zloc.start()
    zsend = [go(remote(e_in, zbuf.at[z], dev(dz=d))) for d in (1, -1, 2)]

    local = []
    local.append(pltpu.make_async_copy(src.at[0], sb.at[pl.ds(0, 256)], loc.at[1]))
    shared = [remote(src.at[0], sb.at[pl.ds(256, 256)], partner)]
    for p in range(2):
        for d in range(4):
            row = pl.multiple_of(p * 1280 + mod(z + d, 4) * 320, 320)
            piece = eo_in.at[pl.ds(row, 320)]
            local.append(pltpu.make_async_copy(piece, eo.at[p * 4 + d, :, pl.ds(0, 256)], loc.at[2 + p * 4 + d]))
            shared.append(remote(piece, eo.at[p * 4 + d, :, pl.ds(256, 256)], partner))
    for copy in local:
        copy.start()
    for copy in shared:
        go(copy)
    dsend = go(remote(depth, d_oth, b_side + (c,)))

    zloc.wait()
    for copy in zsend:
        copy.wait_recv()

    def at16(s):
        place = (x * 4 + y) if s % 2 == 0 else (y * 4 + x)
        return pl.multiple_of(place * 16, 16)

    for s in range(4):
        eb[s, pl.ds(at16(s), 16), :] = zbuf[s, 0:16, :]
    eb[4, pl.ds(at16(4), 16), :] = jnp.concatenate(
        [zbuf[k, 16:20, :].astype(F32) for k in range(4)], axis=0
    ).astype(BF16)

    st = [dict() for _ in range(NS)]

    def small(s):
        rows = eb.at[s, pl.ds(at16(s), 16)]
        mine = zbuf.at[s, pl.ds(0, 16)] if s < 4 else rows
        st[s]["small"] = [
            go(remote(mine, rows, dev(dy=d) if s % 2 == 0 else dev(dx=d))) for d in (1, -1, 2)
        ]

    def along(s, d):
        return dev(dx=d) if s % 2 == 0 else dev(dy=d)

    def line(s, d, first=0, rows=64):
        main = x if s % 2 == 0 else y
        return eb.at[s, pl.ds(pl.multiple_of(mod(main + d + 4, 4) * 64 + first, 16), rows)]

    def large(s):
        for copy in st[s]["small"]:
            copy.wait_recv()
        st[s]["large"] = [go(remote(line(s, 0), line(s, 0), along(s, d))) for d in (1, -1)]

    def forward(s):
        right, left = st[s]["large"]
        right.wait_recv()
        one = go(remote(line(s, -1, 0, 32), line(s, -1, 0, 32), along(s, 1)))
        left.wait_recv()
        two = go(remote(line(s, 1, 32, 32), line(s, 1, 32, 32), along(s, -1)))
        st[s]["forward"] = [one, two]

    def compute(s):
        for copy in st[s]["forward"]:
            copy.wait_recv()
        pt[...] = lax.dot_general(eb[s], sb[...], NT, preferred_element_type=F32).astype(BF16)

        def rows_of(k, _):
            pbuf[s, k] = lax.dot_general(eo[k], pt[...], NT, preferred_element_type=F32).astype(BF16)
            return 0

        lax.fori_loop(0, 8, rows_of, 0)
        right, left = dev(dz=1), dev(dz=-1)
        st[s]["r1"] = go(remote(pbuf.at[s, 2], lbuf.at[s, 0], right))
        st[s]["l1"] = go(remote(pbuf.at[s, 6], rbuf.at[s, 0], left))
        st[s]["r2"] = go(remote(pbuf.at[s, 5], lbuf.at[s, 1], right))
        st[s]["l2"] = go(remote(pbuf.at[s, 3], rbuf.at[s, 1], left))

    def relay(s):
        st[s]["r1"].wait_recv()
        rel[s, 0] = (pbuf[s, 1].astype(F32) + lbuf[s, 0].astype(F32)).astype(BF16)
        st[s]["r3"] = go(remote(rel.at[s, 0], lbuf.at[s, 2], dev(dz=1)))
        st[s]["l1"].wait_recv()
        rel[s, 1] = (pbuf[s, 7].astype(F32) + rbuf[s, 0].astype(F32)).astype(BF16)
        st[s]["l3"] = go(remote(rel.at[s, 1], rbuf.at[s, 2], dev(dz=-1)))

    def part(s, p, k):
        return zf.at[s, p, pl.ds(pl.multiple_of(k * 160, 160), 160)]

    def settle(s):
        for name in ("l2", "r2", "r3", "l3"):
            st[s][name].wait_recv()
        zf[s, 0] = (pbuf[s, 0].astype(F32) + lbuf[s, 2].astype(F32) + rbuf[s, 1].astype(F32)).astype(BF16)
        zf[s, 1] = (pbuf[s, 4].astype(F32) + rbuf[s, 2].astype(F32) + lbuf[s, 1].astype(F32)).astype(BF16)
        st[s]["a1"] = go(remote(part(s, 1 - lo, 1 - hi), ra.at[s, 1], a_side + (c,)))
        st[s]["a0"] = go(remote(part(s, lo, hi), ra.at[s, 0], a_side + (c,)))

    def pair(s):
        st[s]["a1"].wait_recv()
        bs[s] = (part(s, lo, 1 - hi)[...].astype(F32) + ra[s, 1].astype(F32)).astype(BF16)
        st[s]["b"] = go(remote(bs.at[s], xq.at[s, 1], b_side + (c,)))
        st[s]["a0"].wait_recv()
        xq[s, 0] = (part(s, 1 - lo, hi)[...].astype(F32) + ra[s, 0].astype(F32)).astype(BF16)
        st[s]["x0"] = [go(remote(xq.at[s, 0], xg.at[s, k, 0], dev(dx=d))) for k, d in ((0, 1), (1, -1))]

    def second(s):
        st[s]["b"].wait_recv()
        st[s]["x1"] = [go(remote(xq.at[s, 1], xg.at[s, k, 1], dev(dx=d))) for k, d in ((0, 1), (1, -1))]

    def onward(s):
        st[s]["x0"][0].wait_recv()
        st[s]["f0"] = go(remote(xg.at[s, 0, 0], xg.at[s, 2, 0], dev(dx=1)))
        st[s]["x1"][1].wait_recv()
        st[s]["f1"] = go(remote(xg.at[s, 1, 1], xg.at[s, 2, 1], dev(dx=-1)))

    def coefficients():
        dsend.wait_recv()
        column = lax.broadcasted_iota(jnp.int32, (2, 8), 1)
        for h in range(2):
            values = (depth if h == 0 else d_oth)[...]
            for p in range(2):
                half = hi if p == 0 else 1 - hi
                for k, d in enumerate((0, -1, 1, 2)):
                    which = half * 4 + mod(x + d + 4, 4)
                    one = jnp.sum(jnp.where(column == which, values, 0.0), axis=1, keepdims=True)
                    for t in range(2):
                        row = (h * 2 + t) * 8 + p * 4 + k
                        cf[row : row + 1, :] = jnp.broadcast_to(one[t : t + 1, :], (1, 256))

    back = 150

    def mix(s):
        st[s]["x0"][1].wait_recv()
        st[s]["x1"][0].wait_recv()
        st[s]["f0"].wait_recv()
        st[s]["f1"].wait_recv()

        def block(i, _):
            rows = pl.ds(pl.multiple_of(i * 16, 16), 16)
            total = [None] * 4
            for p in range(2):
                for k in range(4):
                    value = (xq[s, p, rows, :] if k == 0 else xg[s, k - 1, p, rows, :]).astype(F32)
                    for g in range(4):
                        row = g * 8 + p * 4 + k
                        term = cf[row : row + 1, :] * value
                        total[g] = term if total[g] is None else total[g] + term
            for g in range(4):
                tb[s, g, rows, :] = total[g].astype(BF16)
            return 0

        lax.fori_loop(0, 10, block, 0)
        place = fin.at[c, s]
        st[s]["t"] = [
            go(remote(tb.at[s, pl.ds(0, 2)], place, a_side + (hi,), slot=back + c * NS + s)),
            go(remote(tb.at[s, pl.ds(2, 2)], place, b_side + (hi,), slot=back + c * NS + s)),
        ]

    def finish(s):
        for k in range(2):
            pltpu.make_async_remote_copy(
                src_ref=tb.at[s, pl.ds(0, 2)], dst_ref=fin.at[k, s], send_sem=send.at[0],
                recv_sem=recv.at[back + k * NS + s],
                device_id=a_side + (c,), device_id_type=pl.DeviceIdType.MESH,
            ).wait_recv()
        r = lax.broadcasted_iota(jnp.int32, (256, 1), 0)
        i = lax.rem(r, 16)
        if s % 2 == 0:
            xx, yy = lax.div(r, 64), lax.rem(lax.div(r, 16), 4)
        else:
            yy, xx = lax.div(r, 64), lax.rem(lax.div(r, 16), 4)
        group = (lax.div(yy, 2) * 4 + xx) * 2 + lax.rem(yy, 2)
        if s < 4:
            target = group * 160 + s * 40 + i
        else:
            target = group * 160 + lax.div(i, 4) * 40 + 16 + lax.rem(i, 4)
        lane = lax.broadcasted_iota(jnp.int32, (256, 256), 1)

        def columns(n, _):
            first = pl.multiple_of(n * 256, 256)
            for t in range(2):
                total = None
                for k in range(2):
                    pick = jnp.where(lane + first == target + k * 20, 1.0, 0.0).astype(BF16)
                    term = jnp.dot(fin[k, s, t], pick, preferred_element_type=F32)
                    total = term if total is None else total + term
                where = (t, slice(None), pl.ds(first, 256))
                out[where] = total if s == 0 else out[where] + total
            return 0

        lax.fori_loop(0, 10, columns, 0)

    small(0); small(1)
    large(0); large(1); small(2); small(3)
    coefficients()
    for copy in local:
        copy.wait()
    forward(0); forward(1); large(2); large(3); small(4)
    for copy in shared:
        copy.wait_recv()
    compute(0); compute(1)
    relay(0); relay(1); forward(2); forward(3); large(4)
    settle(0); settle(1); compute(2); compute(3)
    pair(0); pair(1); relay(2); relay(3); second(0); second(1); forward(4)
    onward(0); onward(1); settle(2); settle(3); compute(4); mix(0); mix(1)
    pair(2); pair(3); relay(4); second(2); second(3); finish(0); finish(1)
    onward(2); onward(3); settle(4); pair(4); mix(2); mix(3); second(4); finish(2); onward(4)
    finish(3); mix(4); finish(4)

    for copy in started:
        copy.wait_send()


def on_device(source, expand_out, expand_in, depth):
    any_space = pl.BlockSpec(memory_space=pl.ANY)
    vmem = pl.BlockSpec(memory_space=pltpu.VMEM)
    return pl.pallas_call(
        kernel,
        out_shape=jax.ShapeDtypeStruct((2, 160, 2560), F32),
        in_specs=[any_space, any_space, any_space, vmem],
        out_specs=vmem,
        scratch_shapes=[
            pltpu.VMEM((4, 20, 4096), BF16),
            pltpu.VMEM((NS, 256, 4096), BF16),
            pltpu.VMEM((512, 4096), BF16),
            pltpu.VMEM((8, 320, 512), BF16),
            pltpu.VMEM((256, 512), BF16),
            pltpu.VMEM((NS, 8, 320, 256), BF16),
            pltpu.VMEM((NS, 3, 320, 256), BF16),
            pltpu.VMEM((NS, 3, 320, 256), BF16),
            pltpu.VMEM((NS, 2, 320, 256), BF16),
            pltpu.VMEM((NS, 2, 320, 256), BF16),
            pltpu.VMEM((NS, 2, 160, 256), BF16),
            pltpu.VMEM((NS, 160, 256), BF16),
            pltpu.VMEM((NS, 2, 160, 256), BF16),
            pltpu.VMEM((NS, 3, 2, 160, 256), BF16),
            pltpu.VMEM((NS, 4, 160, 256), BF16),
            pltpu.VMEM((2, NS, 2, 160, 256), BF16),
            pltpu.VMEM((2, 8), F32),
            pltpu.VMEM((32, 256), F32),
            pltpu.SemaphoreType.DMA((160,)),
            pltpu.SemaphoreType.DMA((160,)),
            pltpu.SemaphoreType.DMA((10,)),
        ],
        compiler_params=pltpu.CompilerParams(
            collective_id=0, has_side_effects=True, vmem_limit_bytes=66 * 1024 * 1024 - 2 * 1024 * 1024 - 70 * 1024,
        ),
    )(source, expand_out, expand_in, depth)


def solution(mesh):
    finer = Mesh(mesh.devices.reshape(2, 4, 2, 4, 2), AXES)
    layer, width = ("hi", "x"), ("lo", "z", "c")
    return jax.shard_map(
        on_device,
        mesh=finer,
        in_specs=(P(layer, width, None), P(None, width), P(layer + width, None), P(layer, None)),
        out_specs=P(layer, width, None),
        check_vma=False,
    )
```
